32 devices in a mesh: gx: 4 (over x, core), gy: 4 (over z), gz: 2 (over y).
Axes of the slice: x: 2, y: 2, z: 4, core: 2. Of those that a mesh axis runs over, the one named last changes fastest.
Arguments:
- occupied: float32 [16, 16, 16, 256], P(None, 'gx', 'gy', 'gz'), may hold values from -6 to 6
- virtual: float32 [16, 16, 16, 256], P(None, 'gx', 'gy', 'gz'), may hold values from -6 to 6
- kernel_fields: float32 [4, 16, 16, 256], P(None, 'gx', 'gy', 'gz'), may hold values from -1.5 to 1.5
- density_grad: float32 [3, 16, 16, 256], P(None, 'gx', 'gy', 'gz'), may hold values from -6 to 6
Outputs:
- potential: float32 [256, 16, 16, 256], P(None, 'gx', 'gy', 'gz')
- casida: float32 [256, 256], P(('gx', 'gy', 'gz'))
The draws below stay inside these ranges and needn't reach their ends.
All inputs are finite; a program needn't handle non-finite values.
Results may differ from the reference program's by a relative error of at most 0.00013.
Values sent between devices are 32-bit elements; how exact they have to be, the bound alone decides.
No kernel may reach another device: no remote copies, remote signals or barrier semaphores. Data moves between devices by JAX's collectives and lax.ppermute only.
A program may use at most 64 MiB of HBM per device.

```python
import jax
import jax.numpy as jnp
from jax import lax

NOCC = 16
NVIR = 16
NX = 16
NY = 16
NZ = 256


def steps_of(rng, extent, split, low, high):
    loudness = 1.0
    for axis_at, blocks in split:
        steps = jax.random.uniform(jax.random.fold_in(jax.random.fold_in(rng, 6), axis_at), (blocks,), jnp.float32, low / len(split), high / len(split))
        loudness = loudness * jnp.repeat(jnp.exp(steps), extent[axis_at] // blocks).reshape((-1,) + (1,) * (len(extent) - 1 - axis_at))
    return loudness


def scatter_about(own_key, extent, scale, most, split=(), held_as=jnp.bfloat16):
    gain = steps_of(own_key, extent, split, -0.22, 0.18) if split else 1.0
    array = jax.random.normal(own_key, extent, jnp.float32) * scale * gain
    return jnp.minimum(jnp.maximum(array, -most), most).astype(held_as)


def setup_inputs(seed: int = 0) -> dict:
    keys = jax.random.split(jax.random.key(seed), 5)
    occupied = scatter_about(keys[0], (NOCC, NX, NY, NZ), 1.0, 6.0, ((1, 4), (2, 4), (3, 2)), jnp.float32)
    virtual = scatter_about(keys[1], (NVIR, NX, NY, NZ), 1.0, 6.0, ((1, 4), (2, 4), (3, 2)), jnp.float32)
    kernel_fields = jnp.clip(jax.random.uniform(keys[2], (4, NX, NY, NZ), jnp.float32, -1.5, 1.5) * steps_of(keys[2], (4, NX, NY, NZ), ((1, 4), (2, 4), (3, 2)), -0.4, 0.0), -1.5, 1.5)
    density_grad = scatter_about(keys[3], (3, NX, NY, NZ), 1.0, 6.0, ((1, 4), (2, 4), (3, 2)), jnp.float32)
    return {"occupied": occupied, "virtual": virtual, "kernel_fields": kernel_fields, "density_grad": density_grad}


def derivative(values, dimension):
    inner_diff = jnp.roll(values, -1, dimension) - jnp.roll(values, 1, dimension)
    outer_diff = jnp.roll(values, -2, dimension) - jnp.roll(values, 2, dimension)
    return (8.0 * inner_diff - outer_diff) / 12.0


def respond(densities, kernel_fields, density_grad):
    slopes = [derivative(densities, dimension + 1) for dimension in range(3)]
    aligned = density_grad[0] * slopes[0] + density_grad[1] * slopes[1] + density_grad[2] * slopes[2]
    scalar = kernel_fields[1] * densities + kernel_fields[2] * aligned
    fluxes = [scalar * density_grad[dimension] + kernel_fields[3] * slopes[dimension] for dimension in range(3)]
    divergence = derivative(fluxes[0], 1) + derivative(fluxes[1], 2) + derivative(fluxes[2], 3)
    return kernel_fields[0] * densities + kernel_fields[1] * aligned - divergence


def reference(occupied, virtual, kernel_fields, density_grad):
    def pair_block(orbital):
        return respond(orbital[None] * virtual, kernel_fields, density_grad)

    potential = lax.map(pair_block, occupied).reshape((NOCC * NVIR, NX, NY, NZ))
    flat_potential = potential.reshape((NOCC * NVIR, NX * NY * NZ))

    def rows_of(orbital):
        densities = (orbital[None] * virtual).reshape((NVIR, NX * NY * NZ))
        return lax.dot_general(densities, flat_potential, (((1,), (1,)), ((), ())), precision=lax.Precision.HIGHEST, preferred_element_type=jnp.float32)

    casida = lax.map(rows_of, occupied).reshape((NOCC * NVIR, NOCC * NVIR)) * (1.0 / (NX * NY * NZ))
    return potential, casida
```

```python
import jax
import jax.numpy as jnp
from jax import lax
from jax.experimental import pallas as pl
from jax.experimental.pallas import tpu as pltpu
from jax.sharding import PartitionSpec as P

REACH = 4
RIM = 2
SHIFTS = (1, -1, 2, -2)


def ring(count, step):
    return [(i, (i + step) % count) for i in range(count)]


def pack_kernel(nx, ny, occ, vir, fields, grad, tile_ref, edge_ref):
    cols = nx * ny
    lanes = tile_ref.shape[-1]
    nvir = vir.shape[0] // cols
    nocc = occ.shape[0] // cols
    half = edge_ref.shape[0] // 2
    per = lanes // REACH
    lane = lax.broadcasted_iota(jnp.int32, tile_ref.shape[1:], 1)
    first = [jnp.zeros(tile_ref.shape[1:], jnp.float32) for _ in range(half)]
    last = [jnp.zeros(tile_ref.shape[1:], jnp.float32) for _ in range(half)]
    used = nvir + nocc + 7
    for c in range(cols):
        tile_ref[c, 0:nvir, :] = vir[pl.ds(c, nvir, stride=cols), :]
        tile_ref[c, nvir : nvir + nocc, :] = occ[pl.ds(c, nocc, stride=cols), :]
        rows = [fields[k * cols + c : k * cols + c + 1, :] for k in range(3)]
        rows.append(fields[3 * cols + c : 3 * cols + c + 1, :] * (1.0 / 144.0))
        rows += [grad[k * cols + c : k * cols + c + 1, :] * (1.0 / 12.0) for k in range(3)]
        for k, row in enumerate(rows):
            tile_ref[c, nvir + nocc + k : nvir + nocc + k + 1, :] = row
        if used < tile_ref.shape[1]:
            tile_ref[c, used:, :] = jnp.zeros((tile_ref.shape[1] - used, lanes), jnp.float32)
        whole = tile_ref[c]
        at, off = c // per, (c % per) * REACH
        here = (lane >= off) & (lane < off + REACH)
        first[at] = jnp.where(here, pltpu.roll(whole, off, 1), first[at])
        last[at] = jnp.where(here, pltpu.roll(whole, (off + REACH) % lanes, 1), last[at])
    for k in range(half):
        edge_ref[k] = first[k]
        edge_ref[half + k] = last[k]


def main_kernel(
    nx, ny, nvir, nocc, scale,
    tile, ends, xlo, xhi, ylo, yhi, clo, chi,
    pot_ref, gram_ref,
    halo, zmid, zhalo, dens, dens_h, flux0, flux1, flux2, flux2h, base,
    dens_hi, dens_lo, pot_hi, pot_lo,
):
    cols = nx * ny
    lanes = tile.shape[-1]
    rows = tile.shape[1]
    orbs = nvir + nocc
    half = ends.shape[0] // 2
    per = lanes // REACH

    def column(x, y):
        if 0 <= x < nx and 0 <= y < ny:
            return tile, x * ny + y
        if 0 <= y < ny:
            return (xlo, (x + REACH) * ny + y) if x < 0 else (xhi, (x - nx) * ny + y)
        if 0 <= x < nx:
            return (ylo, x * REACH + y + REACH) if y < 0 else (yhi, x * REACH + y - ny)
        at = x + RIM if x < 0 else RIM + x - nx
        return (clo, at * RIM + y + RIM) if y < 0 else (chi, at * RIM + y - ny)

    def ends_of(x, y):
        if 0 <= x < nx and 0 <= y < ny:
            return ends, 0, x * ny + y
        if 0 <= y < ny:
            return (xlo, REACH * ny, (x + nx) * ny + y) if x < 0 else (xhi, REACH * ny, (x - nx) * ny + y)
        return (ylo, nx * REACH, x * ny + y + ny) if y < 0 else (yhi, nx * REACH, x * ny + y - ny)

    centre = [(x, y) for x in range(nx) for y in range(ny)]
    cross = list(centre)
    cross += [(x, y) for x in (-2, -1, nx, nx + 1) for y in range(ny)]
    cross += [(x, y) for y in (-2, -1, ny, ny + 1) for x in range(nx)]
    cross_at = {c: k for k, c in enumerate(cross)}
    wide = list(cross)
    wide += [(x, y) for x in (-4, -3, nx + 2, nx + 3) for y in range(ny)]
    wide += [(x, y) for y in (-4, -3, ny + 2, ny + 3) for x in range(nx)]
    wide += [(x, y) for x in (-2, -1, nx, nx + 1) for y in (-2, -1, ny, ny + 1)]
    wide_at = {c: k for k, c in enumerate(wide)}

    def move(mid, out, by):
        lane = lax.broadcasted_iota(jnp.int32, mid.shape, 1)
        a = pltpu.roll(mid, (-by) % lanes, 1)
        b = pltpu.roll(out, (-by) % lanes, 1)
        wraps = lane >= lanes - by if by > 0 else lane < -by
        return jnp.where(wraps, b, a), jnp.where(wraps, a, b)

    for k, (x, y) in enumerate(cross):
        ref, start, c = ends_of(x, y)
        at, off = c // per, (c % per) * REACH
        lane = lax.broadcasted_iota(jnp.int32, (rows, lanes), 1)
        above = pltpu.roll(ref[start + at], (-off) % lanes, 1)
        below = pltpu.roll(ref[start + half + at], (lanes - REACH - off) % lanes, 1)
        out = jnp.where(lane < lanes // 2, above, below)
        halo[k] = out
        ref, c = column(x, y)
        for s, by in enumerate(SHIFTS):
            mid_s, out_s = move(ref[c, 0:orbs, :], out[0:orbs], by)
            gain = 8.0 if abs(by) == 1 else 1.0
            zmid[k, s, 0:nvir, :] = mid_s[0:nvir] * gain
            zmid[k, s, nvir:, :] = mid_s[nvir:]
            if k < cols:
                zhalo[k, s, 0:nvir, :] = out_s[0:nvir] * gain
                zhalo[k, s, nvir:, :] = out_s[nvir:]

    def stencil(p1, m1, p2, m2):
        return 8.0 * (p1 - m1) - (p2 - m2)

    def spread(row):
        return jnp.broadcast_to(row, (nvir, lanes))

    def per_orbital(i, carry):
        row = nvir + i
        pair0 = pl.multiple_of(i * nvir, nvir)
        for k, (x, y) in enumerate(wide):
            ref, c = column(x, y)
            dens[k] = spread(ref[c, pl.ds(row, 1), :]) * ref[c, 0:nvir, :]
        for k in range(len(cross)):
            dens_h[k] = spread(halo[k, pl.ds(row, 1), :]) * halo[k, 0:nvir, :]

        def slope_z(store, k):
            p1, m1, p2, m2 = [
                spread(store[k, s, pl.ds(row, 1), :]) * store[k, s, 0:nvir, :] for s in range(4)
            ]
            return (p1 - m1) - (p2 - m2)

        def respond(d, s0, s1, s2, field):
            g = [field(4 + j) for j in range(3)]
            aligned = g[0] * s0 + g[1] * s1 + g[2] * s2
            scalar = field(1) * d + field(2) * aligned
            return aligned, scalar, g

        for k, (x, y) in enumerate(cross):
            s0 = stencil(*[dens[wide_at[(x + b, y)]] for b in SHIFTS])
            s1 = stencil(*[dens[wide_at[(x, y + b)]] for b in SHIFTS])
            s2 = slope_z(zmid, k)
            ref, c = column(x, y)

            def field(j):
                return spread(ref[c, orbs + j : orbs + j + 1, :])

            d = dens[k]
            aligned, scalar, g = respond(d, s0, s1, s2, field)
            if 0 <= y < ny:
                flux0[(x + RIM) * ny + y] = scalar * g[0] + field(3) * s0
            if 0 <= x < nx:
                flux1[x * (ny + 2 * RIM) + y + RIM] = scalar * g[1] + field(3) * s1
            if k < cols:
                flux2[k] = scalar * g[2] + field(3) * s2
                base[k] = field(0) * d + field(1) * aligned
                s0 = stencil(*[dens_h[cross_at[(x + b, y)]] for b in SHIFTS])
                s1 = stencil(*[dens_h[cross_at[(x, y + b)]] for b in SHIFTS])
                s2 = slope_z(zhalo, k)

                def field_h(j):
                    return spread(halo[k, orbs + j : orbs + j + 1, :])

                aligned, scalar, g = respond(dens_h[k], s0, s1, s2, field_h)
                flux2h[k] = scalar * g[2] + field_h(3) * s2
        for k, (x, y) in enumerate(centre):
            mid, out = flux2[k], flux2h[k]
            total = stencil(*[move(mid, out, b)[0] for b in SHIFTS])
            total += stencil(*[flux0[(x + RIM + b) * ny + y] for b in SHIFTS])
            total += stencil(*[flux1[x * (ny + 2 * RIM) + y + RIM + b] for b in SHIFTS])
            pot = base[k] - total
            pot_ref[pl.ds(pair0 * cols + k, nvir, stride=cols), :] = pot
            there = (pl.ds(pair0, nvir), slice(k * lanes, (k + 1) * lanes))
            top = pot.astype(jnp.bfloat16)
            pot_hi[there] = top
            pot_lo[there] = (pot - top.astype(jnp.float32)).astype(jnp.bfloat16)
            d = dens[k]
            top = d.astype(jnp.bfloat16)
            dens_hi[there] = top
            dens_lo[there] = (d - top.astype(jnp.float32)).astype(jnp.bfloat16)
        return carry

    lax.fori_loop(0, nocc, per_orbital, 0)

    def product(a, b):
        return lax.dot_general(
            a[...], b[...], (((1,), (1,)), ((), ())), preferred_element_type=jnp.float32
        )

    gram = product(dens_hi, pot_lo) + product(dens_lo, pot_hi) + product(dens_hi, pot_hi)
    gram_ref[...] = gram * scale


def on_device(occupied, virtual, kernel_fields, density_grad):
    nocc, nx, ny, nz = occupied.shape
    nvir = virtual.shape[0]
    cols = nx * ny
    rows = -(-(nocc + nvir + 7) // 8) * 8
    half = -(-cols * REACH // nz)
    f32 = jnp.float32
    vmem = pl.BlockSpec(memory_space=pltpu.VMEM)
    axes = ("gx", "gy", "gz")
    devices = lax.axis_size(axes)

    def flat(values):
        return values.reshape((values.shape[0] * cols, nz))

    tile, edges = pl.pallas_call(
        lambda *refs: pack_kernel(nx, ny, *refs),
        out_shape=(
            jax.ShapeDtypeStruct((cols, rows, nz), f32),
            jax.ShapeDtypeStruct((2 * half, rows, nz), f32),
        ),
        in_specs=[vmem] * 4,
        out_specs=(vmem, vmem),
    )(flat(occupied), flat(virtual), flat(kernel_fields), flat(density_grad))

    gz = lax.axis_size("gz")
    if gz == 2:
        ends = lax.ppermute(edges, "gz", ring(gz, 1))
    else:
        ends = jnp.concatenate(
            [
                lax.ppermute(edges[:half], "gz", ring(gz, -1)),
                lax.ppermute(edges[half:], "gz", ring(gz, 1)),
            ]
        )
    gx, gy = lax.axis_size("gx"), lax.axis_size("gy")
    grid = tile.reshape((nx, ny, rows, nz))

    def with_ends(block):
        return jnp.concatenate([block.reshape((-1, rows, nz)), ends])

    xlo = lax.ppermute(with_ends(grid[nx - REACH :]), "gx", ring(gx, 1))
    xhi = lax.ppermute(with_ends(grid[:REACH]), "gx", ring(gx, -1))
    ylo = lax.ppermute(with_ends(grid[:, ny - REACH :]), "gy", ring(gy, 1))
    yhi = lax.ppermute(with_ends(grid[:, :REACH]), "gy", ring(gy, -1))
    rims = jnp.concatenate(
        [xlo[(REACH - RIM) * ny : REACH * ny], xhi[: RIM * ny]]
    ).reshape((2 * RIM, ny, rows, nz))
    clo = lax.ppermute(rims[:, ny - RIM :].reshape((-1, rows, nz)), "gy", ring(gy, 1))
    chi = lax.ppermute(rims[:, :RIM].reshape((-1, rows, nz)), "gy", ring(gy, -1))

    n_cross = cols + 4 * (nx + ny)
    n_wide = n_cross + 4 * (nx + ny) + 16
    pairs = nocc * nvir
    block = (nvir, nz)
    scratch = [
        pltpu.VMEM((n_cross, rows, nz), f32),
        pltpu.VMEM((n_cross, 4, nvir + nocc, nz), f32),
        pltpu.VMEM((cols, 4, nvir + nocc, nz), f32),
        pltpu.VMEM((n_wide,) + block, f32),
        pltpu.VMEM((n_cross,) + block, f32),
        pltpu.VMEM(((nx + 2 * RIM) * ny,) + block, f32),
        pltpu.VMEM((nx * (ny + 2 * RIM),) + block, f32),
        pltpu.VMEM((cols,) + block, f32),
        pltpu.VMEM((cols,) + block, f32),
        pltpu.VMEM((cols,) + block, f32),
    ] + [pltpu.VMEM((pairs, cols * nz), jnp.bfloat16)] * 4
    scale = 1.0 / (cols * nz * devices)
    potential, gram = pl.pallas_call(
        lambda *refs: main_kernel(nx, ny, nvir, nocc, scale, *refs),
        out_shape=(
            jax.ShapeDtypeStruct((pairs * cols, nz), f32),
            jax.ShapeDtypeStruct((pairs, pairs), f32),
        ),
        in_specs=[vmem] * 8,
        out_specs=(vmem, vmem),
        scratch_shapes=scratch,
        compiler_params=pltpu.CompilerParams(vmem_limit_bytes=56 << 20),
    )(tile, ends, xlo, xhi, ylo, yhi, clo, chi)

    parts = lax.all_to_all(gram.reshape((devices, pairs // devices, pairs)), axes, 0, 0)
    casida = jnp.sum(parts, axis=0)
    return potential.reshape((pairs, nx, ny, nz)), casida


def solution(mesh):
    placed = P(None, "gx", "gy", "gz")
    return jax.shard_map(
        on_device,
        mesh=mesh,
        in_specs=(placed,) * 4,
        out_specs=(placed, P(("gx", "gy", "gz"), None)),
        check_vma=False,
    )
```

```python
import jax
import jax.numpy as jnp
from jax import lax
from jax.experimental import pallas as pl
from jax.experimental.pallas import tpu as pltpu
from jax.sharding import PartitionSpec as P


REACH = 4
RIM = 2
SHIFTS = (1, -1, 2, -2)


def ring(count, step):
    return [(i, (i + step) % count) for i in range(count)]


def pack_kernel(nx, ny, occ, vir, fields, grad, tile_ref, edge_ref):
    cols = nx * ny
    lanes = tile_ref.shape[-1]
    nvir = vir.shape[0] // cols
    nocc = occ.shape[0] // cols
    half = edge_ref.shape[0] // 2
    per = lanes // REACH
    lane = lax.broadcasted_iota(jnp.int32, tile_ref.shape[1:], 1)
    first = [jnp.zeros(tile_ref.shape[1:], jnp.float32) for _ in range(half)]
    last = [jnp.zeros(tile_ref.shape[1:], jnp.float32) for _ in range(half)]
    used = nvir + nocc + 7
    for c in range(cols):
        tile_ref[c, 0:nvir, :] = vir[pl.ds(c, nvir, stride=cols), :]
        tile_ref[c, nvir : nvir + nocc, :] = occ[pl.ds(c, nocc, stride=cols), :]
        rows = [fields[k * cols + c : k * cols + c + 1, :] for k in range(3)]
        rows.append(fields[3 * cols + c : 3 * cols + c + 1, :] * (1.0 / 144.0))
        rows += [grad[k * cols + c : k * cols + c + 1, :] * (1.0 / 12.0) for k in range(3)]
        for k, row in enumerate(rows):
            tile_ref[c, nvir + nocc + k : nvir + nocc + k + 1, :] = row
        if used < tile_ref.shape[1]:
            tile_ref[c, used:, :] = jnp.zeros((tile_ref.shape[1] - used, lanes), jnp.float32)
        whole = tile_ref[c]
        at, off = c // per, (c % per) * REACH
        here = (lane >= off) & (lane < off + REACH)
        first[at] = jnp.where(here, pltpu.roll(whole, off, 1), first[at])
        last[at] = jnp.where(here, pltpu.roll(whole, (off + REACH) % lanes, 1), last[at])
    for k in range(half):
        edge_ref[k] = first[k]
        edge_ref[half + k] = last[k]


def main_kernel(
    nx, ny, nvir, nocc, scale,
    tile, ends, xlo, xhi, ynear_lo, ynear_hi, yfar_lo, yfar_hi, yends_lo, yends_hi,
    side_lo, side_hi,
    pot_ref, gram_ref,
    halo, zmid, zhalo, dens, dens_h, flux0, flux1, flux2, flux2h, base,
    dens_hi, dens_lo, pot_hi, pot_lo,
):
    cols = nx * ny
    lanes = tile.shape[-1]
    rows = tile.shape[1]
    orbs = nvir + nocc
    half = ends.shape[0] // 2
    per = lanes // REACH

    def column(x, y):
        if 0 <= x < nx and 0 <= y < ny:
            return tile, x * ny + y
        if 0 <= y < ny:
            return (xlo, (x + REACH) * ny + y) if x < 0 else (xhi, (x - nx) * ny + y)
        if 0 <= x < nx:
            if y < 0:
                return (ynear_lo, x * RIM + y + RIM) if y >= -RIM else (yfar_lo, x * RIM + y + REACH)
            y -= ny
            return (ynear_hi, x * RIM + y) if y < RIM else (yfar_hi, x * RIM + y - RIM)
        ref, at = (side_lo, x + RIM) if x < 0 else (side_hi, x - nx)
        return ref, at * RIM + y + RIM if y < 0 else RIM * RIM + at * RIM + y - ny

    def ends_of(x, y):
        if 0 <= x < nx and 0 <= y < ny:
            return ends, 0, x * ny + y
        if 0 <= y < ny:
            start = 2 * RIM * RIM
            return (side_lo, start, (x + nx) * ny + y) if x < 0 else (side_hi, start, (x - nx) * ny + y)
        return (yends_lo, 0, x * ny + y + ny) if y < 0 else (yends_hi, 0, x * ny + y - ny)

    centre = [(x, y) for x in range(nx) for y in range(ny)]
    cross = list(centre)
    cross += [(x, y) for x in (-2, -1, nx, nx + 1) for y in range(ny)]
    cross += [(x, y) for y in (-2, -1, ny, ny + 1) for x in range(nx)]
    cross_at = {c: k for k, c in enumerate(cross)}
    wide = list(cross)
    wide += [(x, y) for x in (-4, -3, nx + 2, nx + 3) for y in range(ny)]
    wide += [(x, y) for y in (-4, -3, ny + 2, ny + 3) for x in range(nx)]
    wide += [(x, y) for x in (-2, -1, nx, nx + 1) for y in (-2, -1, ny, ny + 1)]
    wide_at = {c: k for k, c in enumerate(wide)}

    def move(mid, out, by):
        lane = lax.broadcasted_iota(jnp.int32, mid.shape, 1)
        a = pltpu.roll(mid, (-by) % lanes, 1)
        b = pltpu.roll(out, (-by) % lanes, 1)
        wraps = lane >= lanes - by if by > 0 else lane < -by
        return jnp.where(wraps, b, a), jnp.where(wraps, a, b)

    for k, (x, y) in enumerate(cross):
        ref, start, c = ends_of(x, y)
        at, off = c // per, (c % per) * REACH
        held = ref.shape[1]
        lane = lax.broadcasted_iota(jnp.int32, (held, lanes), 1)
        above = pltpu.roll(ref[start + at], (-off) % lanes, 1)
        below = pltpu.roll(ref[start + half + at], (lanes - REACH - off) % lanes, 1)
        out = jnp.where(lane < lanes // 2, above, below)
        halo[k, 0:held, :] = out
        ref, c = column(x, y)
        for s, by in enumerate(SHIFTS):
            mid_s, out_s = move(ref[c, 0:orbs, :], out[0:orbs], by)
            gain = 8.0 if abs(by) == 1 else 1.0
            zmid[k, s, 0:nvir, :] = mid_s[0:nvir] * gain
            zmid[k, s, nvir:, :] = mid_s[nvir:]
            if k < cols:
                zhalo[k, s, 0:nvir, :] = out_s[0:nvir] * gain
                zhalo[k, s, nvir:, :] = out_s[nvir:]

    def stencil(p1, m1, p2, m2):
        return 8.0 * (p1 - m1) - (p2 - m2)

    def spread(row):
        return jnp.broadcast_to(row, (nvir, lanes))

    def per_orbital(i, carry):
        row = nvir + i
        pair0 = pl.multiple_of(i * nvir, nvir)
        for k, (x, y) in enumerate(wide):
            ref, c = column(x, y)
            dens[k] = spread(ref[c, pl.ds(row, 1), :]) * ref[c, 0:nvir, :]
        for k in range(len(cross)):
            dens_h[k] = spread(halo[k, pl.ds(row, 1), :]) * halo[k, 0:nvir, :]

        def slope_z(store, k):
            p1, m1, p2, m2 = [
                spread(store[k, s, pl.ds(row, 1), :]) * store[k, s, 0:nvir, :] for s in range(4)
            ]
            return (p1 - m1) - (p2 - m2)

        def respond(d, s0, s1, s2, field):
            g = [field(4 + j) for j in range(3)]
            aligned = g[0] * s0 + g[1] * s1 + g[2] * s2
            scalar = field(1) * d + field(2) * aligned
            return aligned, scalar, g

        for k, (x, y) in enumerate(cross):
            s0 = stencil(*[dens[wide_at[(x + b, y)]] for b in SHIFTS])
            s1 = stencil(*[dens[wide_at[(x, y + b)]] for b in SHIFTS])
            s2 = slope_z(zmid, k)
            ref, c = column(x, y)

            def field(j):
                return spread(ref[c, orbs + j : orbs + j + 1, :])

            d = dens[k]
            aligned, scalar, g = respond(d, s0, s1, s2, field)
            if 0 <= y < ny:
                flux0[(x + RIM) * ny + y] = scalar * g[0] + field(3) * s0
            if 0 <= x < nx:
                flux1[x * (ny + 2 * RIM) + y + RIM] = scalar * g[1] + field(3) * s1
            if k < cols:
                flux2[k] = scalar * g[2] + field(3) * s2
                base[k] = field(0) * d + field(1) * aligned
                s0 = stencil(*[dens_h[cross_at[(x + b, y)]] for b in SHIFTS])
                s1 = stencil(*[dens_h[cross_at[(x, y + b)]] for b in SHIFTS])
                s2 = slope_z(zhalo, k)

                def field_h(j):
                    return spread(halo[k, orbs + j : orbs + j + 1, :])

                aligned, scalar, g = respond(dens_h[k], s0, s1, s2, field_h)
                flux2h[k] = scalar * g[2] + field_h(3) * s2
        for k, (x, y) in enumerate(centre):
            mid, out = flux2[k], flux2h[k]
            total = stencil(*[move(mid, out, b)[0] for b in SHIFTS])
            total += stencil(*[flux0[(x + RIM + b) * ny + y] for b in SHIFTS])
            total += stencil(*[flux1[x * (ny + 2 * RIM) + y + RIM + b] for b in SHIFTS])
            pot = base[k] - total
            pot_ref[pl.ds(pair0 * cols + k, nvir, stride=cols), :] = pot
            there = (pl.ds(pair0, nvir), slice(k * lanes, (k + 1) * lanes))
            top = pot.astype(jnp.bfloat16)
            pot_hi[there] = top
            pot_lo[there] = (pot - top.astype(jnp.float32)).astype(jnp.bfloat16)
            d = dens[k]
            top = d.astype(jnp.bfloat16)
            dens_hi[there] = top
            dens_lo[there] = (d - top.astype(jnp.float32)).astype(jnp.bfloat16)
        return carry

    lax.fori_loop(0, nocc, per_orbital, 0)

    def product(a, b):
        return lax.dot_general(
            a[...], b[...], (((1,), (1,)), ((), ())), preferred_element_type=jnp.float32
        )

    gram = product(dens_hi, pot_lo) + product(dens_lo, pot_hi) + product(dens_hi, pot_hi)
    gram_ref[...] = gram * scale


def on_device(occupied, virtual, kernel_fields, density_grad):
    nocc, nx, ny, nz = occupied.shape
    nvir = virtual.shape[0]
    cols = nx * ny
    rows = -(-(nocc + nvir + 7) // 8) * 8
    half = -(-cols * REACH // nz)
    f32 = jnp.float32
    vmem = pl.BlockSpec(memory_space=pltpu.VMEM)
    axes = ("gx", "gy", "gz")
    devices = lax.axis_size(axes)

    def flat(values):
        return values.reshape((values.shape[0] * cols, nz))

    tile, edges = pl.pallas_call(
        lambda *refs: pack_kernel(nx, ny, *refs),
        out_shape=(
            jax.ShapeDtypeStruct((cols, rows, nz), f32),
            jax.ShapeDtypeStruct((2 * half, rows, nz), f32),
        ),
        in_specs=[vmem] * 4,
        out_specs=(vmem, vmem),
    )(flat(occupied), flat(virtual), flat(kernel_fields), flat(density_grad))

    gz = lax.axis_size("gz")
    if gz == 2:
        ends = lax.ppermute(edges, "gz", ring(gz, 1))
    else:
        ends = jnp.concatenate(
            [
                lax.ppermute(edges[:half], "gz", ring(gz, -1)),
                lax.ppermute(edges[half:], "gz", ring(gz, 1)),
            ]
        )
    gx, gy = lax.axis_size("gx"), lax.axis_size("gy")
    grid = tile.reshape((nx, ny, rows, nz))

    orbs = nocc + nvir

    def stack(*blocks):
        return jnp.concatenate([b[..., :orbs, :].reshape((-1, orbs, nz)) for b in blocks])

    def near(block):
        return block.reshape((-1, rows, nz))

    ynear_lo = lax.ppermute(near(grid[:, ny - RIM :]), "gy", ring(gy, 1))
    ynear_hi = lax.ppermute(near(grid[:, :RIM]), "gy", ring(gy, -1))
    xlo = lax.ppermute(near(grid[nx - REACH :]), "gx", ring(gx, 1))
    xhi = lax.ppermute(near(grid[:REACH]), "gx", ring(gx, -1))
    yfar_lo = lax.ppermute(stack(grid[:, ny - REACH : ny - RIM]), "gy", ring(gy, 1))
    yfar_hi = lax.ppermute(stack(grid[:, RIM:REACH]), "gy", ring(gy, -1))
    yends_lo = lax.ppermute(stack(ends), "gy", ring(gy, 1))
    yends_hi = lax.ppermute(stack(ends), "gy", ring(gy, -1))
    below = ynear_lo.reshape((nx, RIM, rows, nz))
    above = ynear_hi.reshape((nx, RIM, rows, nz))
    side_lo = lax.ppermute(
        stack(below[nx - RIM :], above[nx - RIM :], ends), "gx", ring(gx, 1)
    )
    side_hi = lax.ppermute(stack(below[:RIM], above[:RIM], ends), "gx", ring(gx, -1))

    n_cross = cols + 4 * (nx + ny)
    n_wide = n_cross + 4 * (nx + ny) + 16
    pairs = nocc * nvir
    block = (nvir, nz)
    scratch = [
        pltpu.VMEM((n_cross, rows, nz), f32),
        pltpu.VMEM((n_cross, 4, nvir + nocc, nz), f32),
        pltpu.VMEM((cols, 4, nvir + nocc, nz), f32),
        pltpu.VMEM((n_wide,) + block, f32),
        pltpu.VMEM((n_cross,) + block, f32),
        pltpu.VMEM(((nx + 2 * RIM) * ny,) + block, f32),
        pltpu.VMEM((nx * (ny + 2 * RIM),) + block, f32),
        pltpu.VMEM((cols,) + block, f32),
        pltpu.VMEM((cols,) + block, f32),
        pltpu.VMEM((cols,) + block, f32),
    ] + [pltpu.VMEM((pairs, cols * nz), jnp.bfloat16)] * 4
    scale = 1.0 / (cols * nz * devices)
    potential, gram = pl.pallas_call(
        lambda *refs: main_kernel(nx, ny, nvir, nocc, scale, *refs),
        out_shape=(
            jax.ShapeDtypeStruct((pairs * cols, nz), f32),
            jax.ShapeDtypeStruct((pairs, pairs), f32),
        ),
        in_specs=[vmem] * 12,
        out_specs=(vmem, vmem),
        scratch_shapes=scratch,
        compiler_params=pltpu.CompilerParams(vmem_limit_bytes=56 << 20),
    )(
        tile, ends, xlo, xhi, ynear_lo, ynear_hi, yfar_lo, yfar_hi, yends_lo, yends_hi,
        side_lo, side_hi,
    )

    parts = lax.all_to_all(gram.reshape((devices, pairs // devices, pairs)), axes, 0, 0)
    casida = jnp.sum(parts, axis=0)
    return potential.reshape((pairs, nx, ny, nz)), casida


def solution(mesh):
    placed = P(None, "gx", "gy", "gz")
    return jax.shard_map(
        on_device,
        mesh=mesh,
        in_specs=(placed,) * 4,
        out_specs=(placed, P(("gx", "gy", "gz"), None)),
        check_vma=False,
    )
```

```python
import jax
import jax.numpy as jnp
from jax import lax
from jax.experimental import pallas as pl
from jax.experimental.pallas import tpu as pltpu
from jax.sharding import PartitionSpec as P


REACH = 4
RIM = 2
SHIFTS = (1, -1, 2, -2)


def ring(count, step):
    return [(i, (i + step) % count) for i in range(count)]


def pack_kernel(nx, ny, occ, vir, fields, grad, tile_ref, edge_ref):
    cols = nx * ny
    lanes = tile_ref.shape[-1]
    nvir = vir.shape[0] // cols
    nocc = occ.shape[0] // cols
    half = edge_ref.shape[0] // 2
    per = lanes // REACH
    lane = lax.broadcasted_iota(jnp.int32, tile_ref.shape[1:], 1)
    first = [jnp.zeros(tile_ref.shape[1:], jnp.float32) for _ in range(half)]
    last = [jnp.zeros(tile_ref.shape[1:], jnp.float32) for _ in range(half)]
    used = nvir + nocc + 7
    for c in range(cols):
        tile_ref[c, 0:nvir, :] = vir[pl.ds(c, nvir, stride=cols), :]
        tile_ref[c, nvir : nvir + nocc, :] = occ[pl.ds(c, nocc, stride=cols), :]
        rows = [fields[k * cols + c : k * cols + c + 1, :] for k in range(3)]
        rows.append(fields[3 * cols + c : 3 * cols + c + 1, :] * (1.0 / 144.0))
        rows += [grad[k * cols + c : k * cols + c + 1, :] * (1.0 / 12.0) for k in range(3)]
        for k, row in enumerate(rows):
            tile_ref[c, nvir + nocc + k : nvir + nocc + k + 1, :] = row
        if used < tile_ref.shape[1]:
            tile_ref[c, used:, :] = jnp.zeros((tile_ref.shape[1] - used, lanes), jnp.float32)
        whole = tile_ref[c]
        at, off = c // per, (c % per) * REACH
        here = (lane >= off) & (lane < off + REACH)
        first[at] = jnp.where(here, pltpu.roll(whole, off, 1), first[at])
        last[at] = jnp.where(here, pltpu.roll(whole, (off + REACH) % lanes, 1), last[at])
    for k in range(half):
        edge_ref[k] = first[k]
        edge_ref[half + k] = last[k]


def main_kernel(
    nx, ny, nvir, nocc, scale,
    tile, ends, xlo, xhi, ynear_lo, ynear_hi, yfar_lo, yfar_hi, yends_lo, yends_hi,
    side_lo, side_hi,
    pot_ref, gram_ref,
    halo, zmid, zhalo, dens, dens_h, flux0, flux1, flux2, flux2h, base,
    dens_hi, dens_lo, pot_hi, pot_lo,
):
    cols = nx * ny
    lanes = tile.shape[-1]
    rows = tile.shape[1]
    orbs = nvir + nocc
    half = ends.shape[0] // 2
    per = lanes // REACH

    def column(x, y):
        if 0 <= x < nx and 0 <= y < ny:
            return tile, x * ny + y
        if 0 <= y < ny:
            return (xlo, (x + REACH) * ny + y) if x < 0 else (xhi, (x - nx) * ny + y)
        if 0 <= x < nx:
            if y < 0:
                return (ynear_lo, x * RIM + y + RIM) if y >= -RIM else (yfar_lo, x * RIM + y + REACH)
            y -= ny
            return (ynear_hi, x * RIM + y) if y < RIM else (yfar_hi, x * RIM + y - RIM)
        ref, at = (side_lo, x + RIM) if x < 0 else (side_hi, x - nx)
        return ref, at * RIM + y + RIM if y < 0 else RIM * RIM + at * RIM + y - ny

    def ends_of(x, y):
        if 0 <= x < nx and 0 <= y < ny:
            return ends, 0, x * ny + y
        if 0 <= y < ny:
            start = 2 * RIM * RIM
            return (side_lo, start, (x + nx) * ny + y) if x < 0 else (side_hi, start, (x - nx) * ny + y)
        return (yends_lo, 0, x * ny + y + ny) if y < 0 else (yends_hi, 0, x * ny + y - ny)

    centre = [(x, y) for x in range(nx) for y in range(ny)]
    cross = list(centre)
    cross += [(x, y) for x in (-2, -1, nx, nx + 1) for y in range(ny)]
    cross += [(x, y) for y in (-2, -1, ny, ny + 1) for x in range(nx)]
    cross_at = {c: k for k, c in enumerate(cross)}
    wide = list(cross)
    wide += [(x, y) for x in (-4, -3, nx + 2, nx + 3) for y in range(ny)]
    wide += [(x, y) for y in (-4, -3, ny + 2, ny + 3) for x in range(nx)]
    wide += [(x, y) for x in (-2, -1, nx, nx + 1) for y in (-2, -1, ny, ny + 1)]
    wide_at = {c: k for k, c in enumerate(wide)}

    def move(mid, out, by):
        lane = lax.broadcasted_iota(jnp.int32, mid.shape, 1)
        leaves = lane < by if by > 0 else lane >= lanes + by
        return pltpu.roll(jnp.where(leaves, out, mid), (-by) % lanes, 1)

    for k, (x, y) in enumerate(cross):
        ref, start, c = ends_of(x, y)
        at, off = c // per, (c % per) * REACH
        held = ref.shape[1]
        lane = lax.broadcasted_iota(jnp.int32, (held, lanes), 1)
        above = pltpu.roll(ref[start + at], (-off) % lanes, 1)
        below = pltpu.roll(ref[start + half + at], (lanes - REACH - off) % lanes, 1)
        out = jnp.where(lane < lanes // 2, above, below)
        halo[k, 0:held, :] = out
        ref, c = column(x, y)
        for s, by in enumerate(SHIFTS):
            mid_s = move(ref[c, 0:orbs, :], out[0:orbs], by)
            gain = 8.0 if abs(by) == 1 else 1.0
            zmid[k, s, 0:nvir, :] = mid_s[0:nvir] * gain
            zmid[k, s, nvir:, :] = mid_s[nvir:]
            if k < cols:
                out_s = move(out[0:orbs], ref[c, 0:orbs, :], by)
                zhalo[k, s, 0:nvir, :] = out_s[0:nvir] * gain
                zhalo[k, s, nvir:, :] = out_s[nvir:]

    def stencil(p1, m1, p2, m2):
        return 8.0 * (p1 - m1) - (p2 - m2)

    def spread(row):
        return jnp.broadcast_to(row, (nvir, lanes))

    def per_orbital(i, carry):
        row = nvir + i
        pair0 = pl.multiple_of(i * nvir, nvir)
        for k, (x, y) in enumerate(wide):
            ref, c = column(x, y)
            dens[k] = spread(ref[c, pl.ds(row, 1), :]) * ref[c, 0:nvir, :]
        for k in range(len(cross)):
            dens_h[k] = spread(halo[k, pl.ds(row, 1), :]) * halo[k, 0:nvir, :]

        def slope_z(store, k):
            p1, m1, p2, m2 = [
                spread(store[k, s, pl.ds(row, 1), :]) * store[k, s, 0:nvir, :] for s in range(4)
            ]
            return (p1 - m1) - (p2 - m2)

        def respond(d, s0, s1, s2, field):
            g = [field(4 + j) for j in range(3)]
            aligned = g[0] * s0 + g[1] * s1 + g[2] * s2
            scalar = field(1) * d + field(2) * aligned
            return aligned, scalar, g

        for k, (x, y) in enumerate(cross):
            s0 = stencil(*[dens[wide_at[(x + b, y)]] for b in SHIFTS])
            s1 = stencil(*[dens[wide_at[(x, y + b)]] for b in SHIFTS])
            s2 = slope_z(zmid, k)
            ref, c = column(x, y)

            def field(j):
                return spread(ref[c, orbs + j : orbs + j + 1, :])

            d = dens[k]
            aligned, scalar, g = respond(d, s0, s1, s2, field)
            if 0 <= y < ny:
                flux0[(x + RIM) * ny + y] = scalar * g[0] + field(3) * s0
            if 0 <= x < nx:
                flux1[x * (ny + 2 * RIM) + y + RIM] = scalar * g[1] + field(3) * s1
            if k < cols:
                flux2[k] = scalar * g[2] + field(3) * s2
                base[k] = field(0) * d + field(1) * aligned
                s0 = stencil(*[dens_h[cross_at[(x + b, y)]] for b in SHIFTS])
                s1 = stencil(*[dens_h[cross_at[(x, y + b)]] for b in SHIFTS])
                s2 = slope_z(zhalo, k)

                def field_h(j):
                    return spread(halo[k, orbs + j : orbs + j + 1, :])

                aligned, scalar, g = respond(dens_h[k], s0, s1, s2, field_h)
                flux2h[k] = scalar * g[2] + field_h(3) * s2
        for k, (x, y) in enumerate(centre):
            mid, out = flux2[k], flux2h[k]
            total = stencil(*[move(mid, out, b) for b in SHIFTS])
            total += stencil(*[flux0[(x + RIM + b) * ny + y] for b in SHIFTS])
            total += stencil(*[flux1[x * (ny + 2 * RIM) + y + RIM + b] for b in SHIFTS])
            pot = base[k] - total
            pot_ref[pl.ds(pair0 * cols + k, nvir, stride=cols), :] = pot
            there = (pl.ds(pair0, nvir), slice(k * lanes, (k + 1) * lanes))
            top = pot.astype(jnp.bfloat16)
            pot_hi[there] = top
            pot_lo[there] = (pot - top.astype(jnp.float32)).astype(jnp.bfloat16)
            d = dens[k]
            top = d.astype(jnp.bfloat16)
            dens_hi[there] = top
            dens_lo[there] = (d - top.astype(jnp.float32)).astype(jnp.bfloat16)
        return carry

    lax.fori_loop(0, nocc, per_orbital, 0)

    def product(a, b):
        return lax.dot_general(
            a[...], b[...], (((1,), (1,)), ((), ())), preferred_element_type=jnp.float32
        )

    gram = product(dens_hi, pot_lo) + product(dens_lo, pot_hi) + product(dens_hi, pot_hi)
    gram_ref[...] = gram * scale


def on_device(occupied, virtual, kernel_fields, density_grad):
    nocc, nx, ny, nz = occupied.shape
    nvir = virtual.shape[0]
    cols = nx * ny
    rows = -(-(nocc + nvir + 7) // 8) * 8
    half = -(-cols * REACH // nz)
    f32 = jnp.float32
    vmem = pl.BlockSpec(memory_space=pltpu.VMEM)
    axes = ("gx", "gy", "gz")
    devices = lax.axis_size(axes)

    def flat(values):
        return values.reshape((values.shape[0] * cols, nz))

    tile, edges = pl.pallas_call(
        lambda *refs: pack_kernel(nx, ny, *refs),
        out_shape=(
            jax.ShapeDtypeStruct((cols, rows, nz), f32),
            jax.ShapeDtypeStruct((2 * half, rows, nz), f32),
        ),
        in_specs=[vmem] * 4,
        out_specs=(vmem, vmem),
    )(flat(occupied), flat(virtual), flat(kernel_fields), flat(density_grad))

    gz = lax.axis_size("gz")
    if gz == 2:
        ends = lax.ppermute(edges, "gz", ring(gz, 1))
    else:
        ends = jnp.concatenate(
            [
                lax.ppermute(edges[:half], "gz", ring(gz, -1)),
                lax.ppermute(edges[half:], "gz", ring(gz, 1)),
            ]
        )
    gx, gy = lax.axis_size("gx"), lax.axis_size("gy")
    grid = tile.reshape((nx, ny, rows, nz))

    orbs = nocc + nvir

    def stack(*blocks):
        return jnp.concatenate([b[..., :orbs, :].reshape((-1, orbs, nz)) for b in blocks])

    def near(block):
        return block.reshape((-1, rows, nz))

    ynear_lo = lax.ppermute(near(grid[:, ny - RIM :]), "gy", ring(gy, 1))
    ynear_hi = lax.ppermute(near(grid[:, :RIM]), "gy", ring(gy, -1))
    xlo = lax.ppermute(near(grid[nx - REACH :]), "gx", ring(gx, 1))
    xhi = lax.ppermute(near(grid[:REACH]), "gx", ring(gx, -1))
    yfar_lo = lax.ppermute(stack(grid[:, ny - REACH : ny - RIM]), "gy", ring(gy, 1))
    yfar_hi = lax.ppermute(stack(grid[:, RIM:REACH]), "gy", ring(gy, -1))
    yends_lo = lax.ppermute(stack(ends), "gy", ring(gy, 1))
    yends_hi = lax.ppermute(stack(ends), "gy", ring(gy, -1))
    below = ynear_lo.reshape((nx, RIM, rows, nz))
    above = ynear_hi.reshape((nx, RIM, rows, nz))
    side_lo = lax.ppermute(
        stack(below[nx - RIM :], above[nx - RIM :], ends), "gx", ring(gx, 1)
    )
    side_hi = lax.ppermute(stack(below[:RIM], above[:RIM], ends), "gx", ring(gx, -1))

    n_cross = cols + 4 * (nx + ny)
    n_wide = n_cross + 4 * (nx + ny) + 16
    pairs = nocc * nvir
    block = (nvir, nz)
    scratch = [
        pltpu.VMEM((n_cross, rows, nz), f32),
        pltpu.VMEM((n_cross, 4, nvir + nocc, nz), f32),
        pltpu.VMEM((cols, 4, nvir + nocc, nz), f32),
        pltpu.VMEM((n_wide,) + block, f32),
        pltpu.VMEM((n_cross,) + block, f32),
        pltpu.VMEM(((nx + 2 * RIM) * ny,) + block, f32),
        pltpu.VMEM((nx * (ny + 2 * RIM),) + block, f32),
        pltpu.VMEM((cols,) + block, f32),
        pltpu.VMEM((cols,) + block, f32),
        pltpu.VMEM((cols,) + block, f32),
    ] + [pltpu.VMEM((pairs, cols * nz), jnp.bfloat16)] * 4
    scale = 1.0 / (cols * nz * devices)
    potential, gram = pl.pallas_call(
        lambda *refs: main_kernel(nx, ny, nvir, nocc, scale, *refs),
        out_shape=(
            jax.ShapeDtypeStruct((pairs * cols, nz), f32),
            jax.ShapeDtypeStruct((pairs, pairs), f32),
        ),
        in_specs=[vmem] * 12,
        out_specs=(vmem, vmem),
        scratch_shapes=scratch,
        compiler_params=pltpu.CompilerParams(vmem_limit_bytes=56 << 20),
    )(
        tile, ends, xlo, xhi, ynear_lo, ynear_hi, yfar_lo, yfar_hi, yends_lo, yends_hi,
        side_lo, side_hi,
    )

    parts = lax.all_to_all(gram.reshape((devices, pairs // devices, pairs)), axes, 0, 0)
    casida = jnp.sum(parts, axis=0)
    return potential.reshape((pairs, nx, ny, nz)), casida


def solution(mesh):
    placed = P(None, "gx", "gy", "gz")
    return jax.shard_map(
        on_device,
        mesh=mesh,
        in_specs=(placed,) * 4,
        out_specs=(placed, P(("gx", "gy", "gz"), None)),
        check_vma=False,
    )
```
